32 devices in a mesh: dp: 1, expert: 32 (over z, y, x, core).
Axes of the slice: x: 2, y: 2, z: 4, core: 2. Of those that a mesh axis runs over, the one named last changes fastest.
Arguments:
- tokens: bfloat16 [4096, 1024], P(('dp', 'expert')), may hold values from -6 to 6
- cotangent: bfloat16 [4096, 1024], P(('dp', 'expert')), may hold values from -0.1875 to 0.1875
- expert_ids: int32 [4096, 4], P(('dp', 'expert')), may hold values from 0 to 31, all different within a row; in each aligned block of 128 rows (0 to 127, 128 to 255, ...) at most 32 rows name the same one
- gate_probs: bfloat16 [4096, 4], P(('dp', 'expert')), may hold values from 0.019897461 to 0.59765625
- home_share: int32 [16], replicated, may hold values from 8 to 16
- gate_weight: bfloat16 [32, 1024, 384], P('expert'), may hold values from -0.1875 to 0.1875
- up_weight: bfloat16 [32, 1024, 384], P('expert'), may hold values from -0.1875 to 0.1875
- down_weight: bfloat16 [32, 384, 1024], P('expert'), may hold values from -0.3125 to 0.3125
Outputs:
- gate_cotangent: float32 [4096, 4], P(('dp', 'expert'))
- grad_gate: float32 [32, 1024, 384], P('expert', 'dp')
- grad_up: float32 [32, 1024, 384], P('expert', 'dp')
- grad_down: float32 [32, 384, 1024], P('expert', 'dp')
The draws below stay inside these ranges and needn't reach their ends.
Inputs may be any that keep to these rules, and one draw needn't show every extreme that they name: `expert_ids`: each token names 4 different experts; among the tokens of one device no expert is named more than 32 times.
All inputs are finite; a program needn't handle non-finite values.
Results may differ from the reference program's by a relative error of at most 0.017.
Values may be sent and summed in bfloat16 or wider, within the bound.
No kernel may reach another device: no remote copies, remote signals or barrier semaphores. Data moves between devices by JAX's collectives and lax.ppermute only.
A program may use at most 64 MiB of HBM per device.

```python
import math
import jax
import jax.numpy as jnp
import numpy as np
from jax import lax

D = 1024
FF = 384
TOP = 4
TOK_DEV = 128
EXPERTS = 32
HALF = 16
CAP_OWN = 16
CAP_REP = 4
MOST = 32
TOKENS = 4096
N_DP = 1
N_EXPERT = 32


def place_ends(values, key, least, high):
    index_at = [jax.random.randint(jax.random.fold_in(key, axis), (), 0, length) for axis, length in enumerate(values.shape)]
    main_axis = values.shape.index(max(values.shape))
    beside = index_at[:main_axis] + [(index_at[main_axis] + 1) % values.shape[main_axis]] + index_at[main_axis + 1:]
    return values.at[tuple(index_at)].set(least).at[tuple(beside)].set(high)


def block_scale(key, dims, cuts, least, largest):
    def one(axis_at, parts):
        draws = jax.random.uniform(jax.random.fold_in(jax.random.fold_in(key, 6), axis_at), (parts,), jnp.float32, least / len(cuts), largest / len(cuts))
        return jnp.repeat(jnp.exp(draws), dims[axis_at] // parts).reshape((-1,) + (1,) * (len(dims) - axis_at - 1))

    level = one(*cuts[0])
    for cut in cuts[1:]:
        level = level * one(*cut)
    return level


def routed_block(stream_key, own, number, rows, count, top, limit, lean):
    ranking = jax.random.permutation(stream_key, count)
    crowded, usual = load_shares(count, rows * top, limit, lean, True), load_shares(count, rows * top, limit, lean, False)
    places = jnp.arange(count)

    def named(tallies, rotation):
        used = int((tallies > 0).sum())
        fixed = max(1, used // 4)
        passed = fixed + (places - fixed + rotation * (used - fixed)) % max(1, count - fixed)
        return jnp.zeros((count,), jnp.int32).at[ranking[jnp.where(places < fixed, places, passed)]].set(jnp.asarray(tallies, jnp.int32))

    tallies = jnp.where(number % 4 == 0, named(crowded, number // 4), named(usual, number - number // 4 - 1))
    mixed = jax.random.permutation(jax.random.fold_in(own, 3), count)
    source_of, sink = mixed[0:count // 2 * 2:2], mixed[1:count // 2 * 2:2]
    margin = jnp.minimum(tallies[source_of] - 1, limit - tallies[sink]) // 2
    margin = jnp.where((source_of == ranking[0]) | (sink == ranking[0]) | (tallies[sink] == 0), 0, jnp.maximum(margin, 0))
    passed = jax.random.randint(jax.random.fold_in(own, 4), (count // 2,), 0, 1 << 20) % (margin + 1)
    tallies = tallies.at[source_of].add(-passed).at[sink].add(passed)
    labels = jnp.searchsorted(jnp.cumsum(tallies), jnp.arange(rows * top), side="right").astype(jnp.int32)
    grid = labels.reshape(top, rows).T
    grid = grid[jax.random.permutation(jax.random.fold_in(own, 1), rows)]
    rotation = jax.random.randint(jax.random.fold_in(own, 2), (rows, 1), 0, top)
    return jnp.take_along_axis(grid, (jnp.arange(top)[None, :] + rotation) % top, axis=1)


def load_shares(count, total, reach, lean, full):
    weights = [(1 << 20) // math.isqrt(grade ** lean) + 1 for grade in range(1, count + 1)]
    largest = reach if full else min(reach, max(-(-total // count), total * weights[0] // sum(weights)))
    least = 1 if total - largest >= count - 1 else 0
    given, spare = [largest] + [least] * (count - 1), total - largest - least * (count - 1)
    while spare > 0:
        movable = [i for i in range(1, count) if given[i] < largest] or [i for i in range(1, count) if given[i] < reach]
        mass, budget = sum([weights[i] for i in movable]), spare
        for i in movable:
            extra = min(reach - given[i], max(1, budget * weights[i] // mass), spare)
            given[i] = given[i] + extra
            spare = spare - extra
    return np.array(given)


def scatter_about(own_key, dims, scale, bound, shards=(), held_as=jnp.bfloat16):
    drawn = scale * jax.random.normal(own_key, dims, jnp.float32)
    if shards:
        drawn = drawn * block_scale(own_key, dims, shards, -0.22, 0.18)
    return jnp.clip(drawn, -bound, bound).astype(held_as)


def setup_inputs(seed: int = 0) -> dict:
    keys = jax.random.split(jax.random.key(seed), 9)
    tokens = scatter_about(keys[0], (TOKENS, D), 1.0, 6.0, ((0, 32),))
    cotangent = scatter_about(keys[1], (TOKENS, D), 0.03125, 0.1875, ((0, 32),))
    expert_ids_keys = jax.random.split(jax.random.fold_in(keys[2], 1), TOKENS // TOK_DEV)
    expert_ids_turns = jax.random.permutation(jax.random.fold_in(keys[2], 3), TOKENS // TOK_DEV)
    expert_ids = jax.vmap(lambda own, number: routed_block(jax.random.fold_in(keys[2], 2), own, number, TOK_DEV, EXPERTS, TOP, MOST, 2))(expert_ids_keys, expert_ids_turns).reshape((TOKENS, TOP))
    gate_probs = jnp.clip(jnp.exp(math.log(0.59765625) - 3.4024236 * jax.random.uniform(keys[3], (TOKENS, TOP), jnp.float32) ** block_scale(keys[3], (TOKENS, TOP), ((0, 32),), -0.2, 0.2)), 0.019897461, 0.59765625).astype(jnp.bfloat16)
    home_share = place_ends(jax.random.randint(keys[4], (HALF,), CAP_OWN // 2, CAP_OWN + 1), jax.random.fold_in(keys[4], 1), CAP_OWN // 2, CAP_OWN).astype(jnp.int32)
    gate_weight = scatter_about(keys[5], (EXPERTS, D, FF), D ** -0.5, 0.1875, ((0, 32),))
    up_weight = scatter_about(keys[6], (EXPERTS, D, FF), D ** -0.5, 0.1875, ((0, 32),))
    down_weight = scatter_about(keys[7], (EXPERTS, FF, D), FF ** -0.5, 0.3125, ((0, 32),))
    return {"tokens": tokens, "cotangent": cotangent, "expert_ids": expert_ids, "gate_probs": gate_probs, "home_share": home_share, "gate_weight": gate_weight, "up_weight": up_weight, "down_weight": down_weight}


def route_rows(expert_ids, home_share, experts, cap_own, cap_rep):
    half_axis = experts // 2
    capacity = cap_own + cap_rep
    flat_ids = expert_ids.reshape(-1).astype(jnp.int32)
    columns = jnp.arange(experts, dtype=jnp.int32)
    onehot = (flat_ids[:, None] == columns[None, :]).astype(jnp.int32)
    before = jnp.cumsum(onehot, axis=0) - onehot
    row_rank = jnp.sum(before * onehot, axis=1)
    limits = jnp.concatenate([home_share.astype(jnp.int32), jnp.full((experts - half_axis,), cap_own, jnp.int32)])
    home_limit = jnp.sum(onehot * limits[None, :], axis=1)
    at_home = row_rank < home_limit
    overflow = row_rank - home_limit
    to_copy = (flat_ids < half_axis) & (overflow >= 0) & (overflow < cap_rep)
    target = jnp.where(to_copy, flat_ids + half_axis, flat_ids)
    slot_index = jnp.where(to_copy, cap_own + overflow, row_rank)
    position = jnp.where(at_home | to_copy, target * capacity + slot_index, experts * capacity)
    return position.reshape(expert_ids.shape).astype(jnp.int32)


def dot_exact(left, right):
    return jnp.dot(left.astype(jnp.float32), right.astype(jnp.float32), precision=lax.Precision.HIGHEST)


def expert_side(inputs, grads_out, weights_row, gate_weight, up_weight, down_weight):
    gate_act = dot_exact(inputs, gate_weight)
    up_act = dot_exact(inputs, up_weight)
    sigmoid_gate = jax.nn.sigmoid(gate_act)
    silu_gate = gate_act * sigmoid_gate
    hidden = (silu_gate * up_act).astype(jnp.bfloat16)
    output = dot_exact(hidden, down_weight)
    upstream = grads_out.astype(jnp.float32)
    gate_cot = jnp.sum(upstream * output, axis=1)
    scaled = (weights_row.astype(jnp.float32)[:, None] * upstream).astype(jnp.bfloat16)
    hidden_cot = dot_exact(scaled, down_weight.T)
    gate_pre = (hidden_cot * up_act * sigmoid_gate * (1.0 + gate_act * (1.0 - sigmoid_gate))).astype(jnp.bfloat16)
    up_pre = (hidden_cot * silu_gate).astype(jnp.bfloat16)
    grad_gate = dot_exact(inputs.T, gate_pre)
    grad_up = dot_exact(inputs.T, up_pre)
    grad_down = dot_exact(hidden.T, scaled)
    return gate_cot, grad_gate, grad_up, grad_down


def reference(tokens, cotangent, expert_ids, gate_probs, home_share, gate_weight, up_weight, down_weight):
    experts = EXPERTS
    half_axis = experts // 2
    capacity = CAP_OWN + CAP_REP
    slots_total = N_EXPERT * capacity
    model_width = D

    def pack(tok_block, cot_block, prob_block, position):
        spread = position.shape + (model_width,)
        row_buffer = jnp.zeros((slots_total + 1, model_width), tok_block.dtype)
        row_buffer = row_buffer.at[position].set(jnp.broadcast_to(tok_block[:, None, :], spread))
        cot_buffer = jnp.zeros((slots_total + 1, model_width), cot_block.dtype)
        cot_buffer = cot_buffer.at[position].set(jnp.broadcast_to(cot_block[:, None, :], spread))
        prob_buffer = jnp.zeros((slots_total + 1,), prob_block.dtype).at[position].set(prob_block)
        return row_buffer[:-1], cot_buffer[:-1], prob_buffer[:-1]

    def group_step(totals, group):
        tok_group, cot_group, id_group, prob_group = group
        positions = jax.vmap(lambda blocks: route_rows(blocks, home_share, experts, CAP_OWN, CAP_REP))(id_group)
        send_rows, send_cots, send_probs = jax.vmap(pack)(tok_group, cot_group, prob_group, positions)
        recv_rows = jnp.swapaxes(send_rows.reshape(N_EXPERT, N_EXPERT, capacity, model_width), 0, 1)
        recv_cots = jnp.swapaxes(send_cots.reshape(N_EXPERT, N_EXPERT, capacity, model_width), 0, 1)
        recv_probs = jnp.swapaxes(send_probs.reshape(N_EXPERT, N_EXPERT, capacity), 0, 1)

        def device_step(device):
            slot_rows = recv_rows[device]
            slot_cots = recv_cots[device]
            slot_probs = recv_probs[device]
            home_part = expert_side(slot_rows[:, :CAP_OWN].reshape(-1, model_width), slot_cots[:, :CAP_OWN].reshape(-1, model_width), slot_probs[:, :CAP_OWN].reshape(-1), gate_weight[device], up_weight[device], down_weight[device])
            source = (device - half_axis) % experts
            copy_part = expert_side(slot_rows[:, CAP_OWN:].reshape(-1, model_width), slot_cots[:, CAP_OWN:].reshape(-1, model_width), slot_probs[:, CAP_OWN:].reshape(-1), gate_weight[source], up_weight[source], down_weight[source])
            gate_cot = jnp.concatenate([home_part[0].reshape(N_EXPERT, CAP_OWN), copy_part[0].reshape(N_EXPERT, CAP_REP)], axis=1)
            return gate_cot, home_part[1:], copy_part[1:]

        gate_cot, home_grads, copy_grads = lax.map(device_step, jnp.arange(experts, dtype=jnp.int32))
        returned = jnp.swapaxes(gate_cot, 0, 1).reshape(N_EXPERT, slots_total)

        def unpack(back_row, position):
            return jnp.concatenate([back_row, jnp.zeros((1,), jnp.float32)])[position]

        group_cot = jax.vmap(unpack)(returned, positions)
        new_totals = []
        for total, home_grad, copy_grad in zip(totals, home_grads, copy_grads):
            copy_bf = lax.optimization_barrier(copy_grad.astype(jnp.bfloat16)).astype(jnp.float32)
            home_bf = lax.optimization_barrier(home_grad.astype(jnp.bfloat16)).astype(jnp.float32)
            at_home = jnp.concatenate([copy_bf[half_axis:], jnp.zeros_like(copy_bf[:experts - half_axis])])
            new_totals.append(total + home_bf + at_home)
        return tuple(new_totals), group_cot

    def shaped(array):
        return array.reshape((N_DP, N_EXPERT, TOK_DEV) + array.shape[1:])

    start = (jnp.zeros((experts, D, FF), jnp.float32), jnp.zeros((experts, D, FF), jnp.float32), jnp.zeros((experts, FF, D), jnp.float32))
    totals, group_cots = lax.scan(group_step, start, (shaped(tokens), shaped(cotangent), shaped(expert_ids), shaped(gate_probs)))
    return group_cots.reshape(TOKENS, TOP), totals[0], totals[1], totals[2]
```

```python
import functools
import jax
import jax.numpy as jnp
from jax import lax
from jax.experimental import pallas as pl
from jax.experimental.pallas import tpu as pltpu
from jax.sharding import PartitionSpec as P

BF16 = jnp.bfloat16
F32 = jnp.float32
VMEM = pl.BlockSpec(memory_space=pltpu.VMEM)
SMEM = pl.BlockSpec(memory_space=pltpu.SMEM)


def slot_plan(cap):
    main = cap // 8 * 8
    rest = cap - main
    return main, rest, 2 * main + -(-2 * rest // 8) * 8


def ranks(ids, share_ref, base, count, half, cap_own, cap_rep):
    tokens = ids.shape[1]
    expert = base + lax.broadcasted_iota(jnp.int32, (count, tokens), 0)
    named = jnp.zeros((count, tokens), F32)
    for choice in range(ids.shape[0]):
        named = named + jnp.where(ids[choice : choice + 1, :] == expert, 1.0, 0.0)
    earlier = lax.broadcasted_iota(jnp.int32, (tokens, tokens), 0) < lax.broadcasted_iota(
        jnp.int32, (tokens, tokens), 1
    )
    rank = jnp.dot(
        named.astype(BF16), jnp.where(earlier, 1.0, 0.0).astype(BF16), preferred_element_type=F32
    )
    limit = jnp.full((count, tokens), cap_own, jnp.int32)
    for index in range(half):
        limit = jnp.where(expert == index, share_ref[index] + cap_rep, limit)
    kept = (named > 0.5) & (rank < limit.astype(F32))
    return expert, jnp.where(kept, rank, -1.0)


def pack_rows(ids, probs, data, share_ref, base, count, half, cap_own, cap_rep):
    main, rest, chunk = slot_plan(cap_own + cap_rep)
    tokens = ids.shape[1]
    expert, rank = ranks(ids, share_ref, base, count, half, cap_own, cap_rep)
    weight = jnp.zeros((count, tokens), F32)
    for choice in range(ids.shape[0]):
        weight = weight + jnp.where(ids[choice : choice + 1, :] == expert, probs[choice : choice + 1, :], 0.0)
    line = lax.broadcasted_iota(jnp.int32, (chunk, tokens), 0)
    tail = line - 2 * main
    row_slot = jnp.where(line < main, line, jnp.where((tail >= 0) & (tail < rest), main + tail, -2))
    cot_slot = jnp.where(
        (line >= main) & (line < 2 * main),
        line - main,
        jnp.where((tail >= rest) & (tail < 2 * rest), main + tail - rest, -2),
    )
    row_slot, cot_slot = row_slot.astype(F32), cot_slot.astype(F32)
    left, right = [], []
    for index in range(count):
        own = rank[index : index + 1, :]
        left.append(jnp.where(own == row_slot, 1.0, 0.0))
        right.append(jnp.where(own == cot_slot, weight[index : index + 1, :], 0.0))
    pick = jnp.concatenate([jnp.concatenate(left, 0), jnp.concatenate(right, 0)], 1).astype(BF16)
    return jnp.dot(pick, data, preferred_element_type=F32).astype(BF16)


def own_pack_kernel(caps, ids_ref, probs_ref, share_ref, data_ref, out_ref):
    half, cap_own, cap_rep, tokens = caps
    base = lax.axis_index("expert") // half * half
    out_ref[...] = pack_rows(
        ids_ref[...], probs_ref[...].astype(F32), data_ref[: 2 * tokens, :], share_ref, base, half, half, cap_own, cap_rep
    )


def far_pack_kernel(caps, share_ref, outer_ref, inner_ref, out_ref):
    half, cap_own, cap_rep, tokens, top = caps
    me = lax.axis_index("expert")
    base = me // half * half
    block = me // (half // 2)
    outer = jnp.where((block == 0) | (block == 3), 1, 0)
    data = jnp.where(outer == 1, outer_ref[...], inner_ref[...])
    meta = data[2 * tokens :, :tokens].astype(F32)
    out_ref[...] = pack_rows(
        meta[:top].astype(jnp.int32), meta[top : 2 * top], data[: 2 * tokens, :], share_ref, base, half, half, cap_own, cap_rep
    )


def quotient(value, by):
    return jnp.floor((value.astype(F32) + 0.5) / by)


def expert_rows(cap, recv_ref, gate_ref, up_ref, down_ref):
    main, rest, chunk = slot_plan(cap)
    sources = recv_ref.shape[0]
    width = recv_ref.shape[2]
    inputs = recv_ref[:, :main, :].astype(F32).reshape(sources * main, width).astype(BF16)
    scaled = recv_ref[:, main : 2 * main, :].astype(F32).reshape(sources * main, width).astype(BF16)
    if rest:
        extra = chunk - 2 * main
        mixed = recv_ref[:, 2 * main :, :].astype(F32).reshape(sources * extra, width).astype(BF16)
        shape = (sources * rest, sources * extra)
        row = lax.broadcasted_iota(jnp.int32, shape, 0).astype(F32)
        column = lax.broadcasted_iota(jnp.int32, shape, 1).astype(F32)
        source = quotient(row, rest)
        wanted = source * extra + (row - source * rest)
        pick_rows = jnp.where(column == wanted, 1.0, 0.0).astype(BF16)
        pick_cots = jnp.where(column == wanted + rest, 1.0, 0.0).astype(BF16)
        inputs = jnp.concatenate([inputs, jnp.dot(pick_rows, mixed, preferred_element_type=F32).astype(BF16)], 0)
        scaled = jnp.concatenate([scaled, jnp.dot(pick_cots, mixed, preferred_element_type=F32).astype(BF16)], 0)
    gate_act = jnp.dot(inputs, gate_ref[...], preferred_element_type=F32)
    up_act = jnp.dot(inputs, up_ref[...], preferred_element_type=F32)
    hidden_cot = lax.dot_general(scaled, down_ref[...], (((1,), (1,)), ((), ())), preferred_element_type=F32)
    sigmoid = 1.0 / (1.0 + jnp.exp(-gate_act))
    silu = gate_act * sigmoid
    hidden = (silu * up_act).astype(BF16)
    gate_pre = (hidden_cot * up_act * sigmoid * (1.0 + gate_act * (1.0 - sigmoid))).astype(BF16)
    up_pre = (hidden_cot * silu).astype(BF16)
    dots = jnp.sum(hidden.astype(F32) * hidden_cot, axis=1, keepdims=True)
    total = sources * cap
    row = lax.broadcasted_iota(jnp.int32, (total, 128), 0).astype(F32)
    lane = lax.broadcasted_iota(jnp.int32, (total, 128), 1).astype(F32)
    edge = float(sources * main)
    slot = jnp.where(row < edge, row - quotient(row, main) * main, main + (row - edge) - quotient(row - edge, max(rest, 1)) * rest)
    spread = jnp.where(lane == slot, dots, 0.0)
    row = lax.broadcasted_iota(jnp.int32, (sources, total), 1).astype(F32)
    source = jnp.where(row < edge, quotient(row, main), quotient(row - edge, max(rest, 1)))
    mine = jnp.where(source == lax.broadcasted_iota(jnp.int32, (sources, total), 0).astype(F32), 1.0, 0.0)
    table = jnp.dot(mine, spread, precision=lax.Precision.HIGHEST, preferred_element_type=F32)
    return inputs, scaled, gate_pre, up_pre, hidden, table


def near_kernel(cap, recv_ref, gate_ref, up_ref, down_ref, *out_refs):
    for ref, part in zip(out_refs, expert_rows(cap, recv_ref, gate_ref, up_ref, down_ref)):
        ref[...] = part


def far_kernel(cap, recv_ref, gate_ref, up_ref, down_ref, near_ref, *out_refs):
    half = recv_ref.shape[0]
    quarter = half // 2
    parts = expert_rows(cap, recv_ref, gate_ref, up_ref, down_ref)
    for ref, part in zip(out_refs, parts[:5]):
        ref[...] = part
    table, table_ref = parts[5], out_refs[5]
    base = pl.multiple_of(lax.axis_index("expert") // half * half, 8)
    other = pl.multiple_of(half - base, 8)
    table_ref[pl.ds(base, half), :] = near_ref[...]
    table_ref[pl.ds(other, half), :] = jnp.concatenate([table[quarter:], table[:quarter]], 0)


def grad_kernel(x1, x2, s1, s2, g1, g2, u1, u2, h1, h2, gate_ref, up_ref, down_ref):
    step = pl.program_id(0)
    block = gate_ref.shape[0]
    part = down_ref.shape[1]
    columns = pl.ds(pl.multiple_of(step * block, 128), block)

    def product(left, right):
        return lax.dot_general(left, right, (((0,), (0,)), ((), ())), preferred_element_type=F32)

    x = jnp.concatenate([x1[:, columns], x2[:, columns]], 0)
    gate_ref[...] = product(x, jnp.concatenate([g1[...], g2[...]], 0))
    up_ref[...] = product(x, jnp.concatenate([u1[...], u2[...]], 0))
    columns = pl.ds(pl.multiple_of(step * part, 128), part)
    s = jnp.concatenate([s1[:, columns], s2[:, columns]], 0)
    down_ref[...] = product(jnp.concatenate([h1[...], h2[...]], 0), s)


def finish_kernel(caps, ids_ref, probs_ref, share_ref, table_ref, out_ref):
    half, cap_own, cap_rep = caps
    ids = ids_ref[...]
    table = table_ref[...]
    count = table.shape[0]
    expert, rank = ranks(ids, share_ref, 0, count, half, cap_own, cap_rep)
    found = jnp.zeros(rank.shape, F32)
    for slot in range(cap_own + cap_rep):
        found = found + jnp.where(rank == float(slot), table[:, slot : slot + 1], 0.0)
    lines = []
    for choice in range(ids.shape[0]):
        lines.append(jnp.sum(jnp.where(ids[choice : choice + 1, :] == expert, found, 0.0), axis=0, keepdims=True))
    out_ref[...] = jnp.concatenate(lines, 0) / probs_ref[...].astype(F32)


def call(kernel, outs, in_specs):
    return pl.pallas_call(
        kernel,
        out_shape=outs,
        in_specs=in_specs,
        out_specs=jax.tree.map(lambda _: VMEM, outs),
        compiler_params=pltpu.CompilerParams(vmem_limit_bytes=48 * 1024 * 1024),
    )


def per_device(
    tokens, cotangent, expert_ids, gate_probs, home_share, gate_weight, up_weight, down_weight
):
    experts = lax.axis_size("expert")
    rows, width = tokens.shape
    top = expert_ids.shape[1]
    cap_own = rows * top // experts
    cap_rep = cap_own // 4
    cap = cap_own + cap_rep
    half = experts // 2
    quarter = experts // 4
    hidden_units = gate_weight.shape[2]
    chunk = slot_plan(cap)[2]
    groups = [list(range(half)), list(range(half, experts))]
    mirror = [(e, (3 - e // quarter) * quarter + e % quarter) for e in range(experts)]
    outer = [pair for pair in mirror if pair[0] // quarter in (0, 3)]
    inner = [pair for pair in mirror if pair[0] // quarter in (1, 2)]
    struct = jax.ShapeDtypeStruct

    ids, probs = expert_ids.T, gate_probs.T
    meta = jnp.concatenate([ids.astype(BF16), probs], 0)
    meta = jnp.pad(meta, ((0, -2 * top % 8), (0, width - rows)))
    data = jnp.concatenate([tokens, cotangent, meta], 0)
    far_outer = lax.ppermute(data, "expert", outer)
    near_send = call(
        functools.partial(own_pack_kernel, (half, cap_own, cap_rep, rows)),
        struct((half * chunk, width), BF16),
        [VMEM, VMEM, SMEM, VMEM],
    )(ids, probs, home_share, data)
    near_send, data = lax.optimization_barrier((near_send, data))
    exchange = functools.partial(
        lax.all_to_all, axis_name="expert", split_axis=0, concat_axis=0, axis_index_groups=groups, tiled=True
    )
    near = exchange(near_send.reshape(half, chunk, width))
    far_inner = lax.ppermute(data, "expert", inner)
    far_send = call(
        functools.partial(far_pack_kernel, (half, cap_own, cap_rep, rows, top)),
        struct((half * chunk, width), BF16),
        [SMEM, VMEM, VMEM],
    )(home_share, far_outer, far_inner)
    far = exchange(far_send.reshape(half, chunk, width))

    weights = (gate_weight[0], up_weight[0], down_weight[0])
    total = half * cap
    kept = (
        struct((total, width), BF16),
        struct((total, width), BF16),
        struct((total, hidden_units), BF16),
        struct((total, hidden_units), BF16),
        struct((total, hidden_units), BF16),
    )
    first = call(functools.partial(near_kernel, cap), kept + (struct((half, 128), F32),), [VMEM] * 4)(near, *weights)
    second = call(functools.partial(far_kernel, cap), kept + (struct((experts, 128), F32),), [VMEM] * 5)(
        far, *weights, first[5]
    )
    back = lax.all_to_all(
        second[5].reshape(experts, 1, 128), "expert", split_axis=0, concat_axis=0, tiled=True
    ).reshape(experts, 128)
    steps = 4
    grads = pl.pallas_call(
        grad_kernel,
        grid=(steps,),
        out_shape=(
            struct((width, hidden_units), F32),
            struct((width, hidden_units), F32),
            struct((hidden_units, width), F32),
        ),
        in_specs=[VMEM] * 10,
        out_specs=(
            pl.BlockSpec((width // steps, hidden_units), lambda i: (i, 0)),
            pl.BlockSpec((width // steps, hidden_units), lambda i: (i, 0)),
            pl.BlockSpec((hidden_units, width // steps), lambda i: (0, i)),
        ),
    )(*[part for pair in zip(first[:5], second[:5]) for part in pair])
    gate_cot = call(
        functools.partial(finish_kernel, (half, cap_own, cap_rep)),
        struct((top, rows), F32),
        [VMEM, VMEM, SMEM, VMEM],
    )(ids, probs, home_share, back).T
    if lax.axis_size("dp") > 1:
        grads = tuple(
            lax.psum_scatter(grad.astype(BF16), "dp", scatter_dimension=0, tiled=True).astype(F32) for grad in grads
        )
    return (gate_cot, grads[0][None], grads[1][None], grads[2][None])


def solution(mesh):
    return jax.shard_map(
        per_device,
        mesh=mesh,
        in_specs=(
            P(("dp", "expert"), None),
            P(("dp", "expert"), None),
            P(("dp", "expert"), None),
            P(("dp", "expert"), None),
            P(),
            P("expert", None, None),
            P("expert", None, None),
            P("expert", None, None),
        ),
        out_specs=(
            P(("dp", "expert"), None),
            P("expert", "dp", None),
            P("expert", "dp", None),
            P("expert", "dp", None),
        ),
        check_vma=False,
    )
```
